16 devices in a mesh: rep: 1, r: 2 (over z), s: 8 (over x, y, core).
Axes of the slice: x: 2, y: 2, z: 2, core: 2. Of those that a mesh axis runs over, the one named last changes fastest.
Arguments:
- x: bfloat16 [16, 2048, 768], P(('rep', 'r', 's'))
- dy: bfloat16 [16, 2048, 768], P(('rep', 'r', 's'))
- w_gate: bfloat16 [2, 768, 6144], P(None, 's')
- w_up: bfloat16 [2, 768, 6144], P(None, 's')
- w_down: bfloat16 [2, 6144, 768], P(None, 's')
Outputs:
- output 1: bfloat16 [16, 2048, 768], P(('rep', 'r', 's'))
- output 2: bfloat16 [2, 768, 6144], P('rep', 's')
- output 3: bfloat16 [2, 768, 6144], P('rep', 's')
- output 4: bfloat16 [2, 6144, 768], P('rep', 's')
All inputs are finite; a program needn't handle non-finite values.
Results may differ from the reference program's by a relative error of at most 0.018.
Values are sent between devices in bfloat16 or wider.
A program may use at most 2 GiB of HBM per device.

```python
import jax
import jax.numpy as jnp
from jax import lax

SEQUENCES = 16
TOKENS = 2048
D = 768
FF = 6144
LAYERS = 2
NAMES = ("w_gate", "w_up", "w_down")
SHAPES = {"w_gate": (LAYERS, D, FF), "w_up": (LAYERS, D, FF), "w_down": (LAYERS, FF, D)}


def bump(key, n, height):
    away = (jnp.arange(n, dtype=jnp.int32) - jax.random.randint(key, (), 0, n, jnp.int32)) % n
    return jnp.where(away < n // 8, height, 1.0)


def together(key, own, strength):
    shared = jax.random.normal(key, own.shape[1:], jnp.float32)
    return (own + strength * shared) * lax.rsqrt(1 + strength * strength)


def setup_inputs(seed: int = 0, part: int = 0) -> dict:
    kx, kdy, ka, kb, kz, kf, kh, kl, *kw = jax.random.split(jax.random.key(seed), 8 + len(NAMES))
    kx, kdy, ka, kb = (jax.random.fold_in(k, part) for k in (kx, kdy, ka, kb))
    shape = (SEQUENCES, TOKENS, D)
    much_x, much_dy = jax.random.uniform(kz, (2,), jnp.float32, 0.0, 1.0)
    layers = 2.0 ** jax.random.uniform(kl, (LAYERS, 1, 1), jnp.float32, -1.0, 1.0)
    x = together(ka, jax.random.normal(kx, shape, jnp.float32), much_x) * bump(kf, D, 4.0)
    dy = together(kb, jax.random.normal(kdy, shape, jnp.float32), much_dy)
    drawn = {"x": x.astype(jnp.bfloat16), "dy": (dy * (SEQUENCES * TOKENS) ** -0.5).astype(jnp.bfloat16)}
    for key, name in zip(kw, NAMES, strict=True):
        w = jax.random.normal(key, SHAPES[name], jnp.float32) * SHAPES[name][1] ** -0.5
        drawn[name] = (w * {"w_gate": 1.0, "w_up": bump(kh, FF, 4.0), "w_down": layers}[name]).astype(jnp.bfloat16)
    return drawn


def matmul(a, w):
    return jnp.dot(a, w, preferred_element_type=jnp.float32).astype(jnp.bfloat16)


def normed(h):
    wide = h.astype(jnp.float32)
    scale = lax.rsqrt(jnp.mean(wide**2, -1, keepdims=True) + 1e-6)
    return (wide * scale).astype(jnp.bfloat16)


def layer(h, w):
    a = normed(h)
    gate = jnp.dot(a, w["w_gate"], preferred_element_type=jnp.float32)
    up = jnp.dot(a, w["w_up"], preferred_element_type=jnp.float32)
    return h + matmul((jax.nn.silu(gate) * up).astype(jnp.bfloat16), w["w_down"])


def stack(weights, h):
    return lax.scan(lambda h, w: (layer(h, w), None), h, weights)[0]


def reference(x, dy, w_gate, w_up, w_down):
    weights = dict(zip(NAMES, (w_gate, w_up, w_down), strict=True))

    def take(so_far, sequence):
        h, by_y = sequence
        _, back = jax.vjp(stack, weights, h)
        by_weights, by_h = back(by_y)
        return jax.tree.map(lambda total, term: total + term.astype(jnp.float32), so_far, by_weights), by_h

    none_yet = {name: jnp.zeros(w.shape, jnp.float32) for name, w in weights.items()}
    by_weights, by_x = lax.scan(take, none_yet, (x, dy))
    return (by_x, *(by_weights[name].astype(jnp.bfloat16) for name in NAMES))
```

```python
import functools

import jax
import jax.numpy as jnp
from jax import lax
from jax.experimental import pallas as pl
from jax.experimental.pallas import tpu as pltpu
from jax.sharding import PartitionSpec as P

MESH = pl.DeviceIdType.MESH
BF, F32 = jnp.bfloat16, jnp.float32
J = 6
TILES = 4


def nn(a, b):
    return lax.dot_general(a, b, (((1,), (0,)), ((), ())), preferred_element_type=F32)


def nt(a, b):
    return lax.dot_general(a, b, (((1,), (1,)), ((), ())), preferred_element_type=F32)


def kernel(
    x_ref, dy_ref, gu_ref, wd_ref,
    dx_ref, out_ref, g_ref, d_ref, h_ref,
    a, at, dy, dyt, acc, guv, wdv, mid, dg, du, term, r1, r2, r3, r4,
    ag_recv, ag_send, load_sem, s1, s2, s3, s4, out_sem, io_sem,
):
    tokens, width = a.shape
    rows = tokens // TILES
    U = 2 * J
    r, s = lax.axis_index("r"), lax.axis_index("s")
    c, y, x = s % 2, (s // 2) % 2, s // 4
    xy = s // 2
    partner, xn, yn = s + 1 - 2 * c, s + 4 - 8 * x, s + 2 - 4 * y
    dev_p, dev_x, dev_y, dev_z = {"s": partner}, {"s": xn}, {"s": yn}, {"r": 1 - r}
    dev_1 = {"s": xn * (1 - r) + yn * r}
    dev_2 = {"s": xn * r + yn * (1 - r)}
    pos1 = xy + (1 - r) * (2 - 4 * x) + r * (1 - 2 * y)
    pos2 = xy + r * (2 - 4 * x) + (1 - r) * (1 - 2 * y)
    pos3 = 3 - xy

    def remote(src, dst, send, recv, dev):
        return pltpu.make_async_remote_copy(src_ref=src, dst_ref=dst, send_sem=send, recv_sem=recv, device_id=dev, device_id_type=MESH)

    def pieces(u, pos, own):
        if own:
            return (gu_ref.at[u], wd_ref.at[u])
        return (g_ref.at[u, pos, c], d_ref.at[u, pos, c])

    def send_block(u, pos, own, kind, dev):
        for i, (src, dst) in enumerate(zip(pieces(u, pos, own), (g_ref.at[u, pos, c], d_ref.at[u, pos, c]))):
            remote(src, dst, ag_send.at[u, 1 if kind == 3 else 0, i], ag_recv.at[u, kind, i], dev).start()

    def wait_block(u, pos, kind):
        for i, ref in enumerate((g_ref.at[u, pos, c], d_ref.at[u, pos, c])):
            remote(ref, ref, ag_send.at[u, 0, i], ag_recv.at[u, kind, i], dev_1).wait_recv()

    def hop(u):
        send_block(u, xy, True, 0, dev_1)

    def forward(u):
        send_block(u, xy, True, 3, dev_p)
        wait_block(u, pos1, 0)
        send_block(u, pos1, False, 1, dev_2)
        send_block(u, pos1, False, 2, dev_z)
        send_block(u, pos1, False, 3, dev_p)

    def across(u):
        wait_block(u, pos2, 2)
        send_block(u, pos2, False, 3, dev_p)
        wait_block(u, pos3, 1)
        send_block(u, pos3, False, 3, dev_p)

    def arrived(u):
        for i, ref in enumerate((g_ref.at[u, :, 1 - c], d_ref.at[u, :, 1 - c])):
            remote(ref, ref, ag_send.at[u, 1, i], ag_recv.at[u, 3, i], dev_p).wait_recv()

    def sent(u):
        for i, ref in enumerate((g_ref, d_ref)):
            three, four = ref.at[u, pl.ds(0, 3), 0], ref.at[u, :, 0]
            remote(three, three, ag_send.at[u, 0, i], ag_recv.at[u, 0, i], dev_1).wait_send()
            remote(four, four, ag_send.at[u, 1, i], ag_recv.at[u, 3, i], dev_p).wait_send()

    def load(u, slot):
        for i, (own, all_, to) in enumerate(((gu_ref, g_ref, guv), (wd_ref, d_ref, wdv))):
            sem = load_sem.at[slot, i]
            pltpu.make_async_copy(own.at[u], to.at[slot, xy, c], sem).start()
            for pos in (pos1, pos2, pos3):
                pltpu.make_async_copy(all_.at[u, pos, c], to.at[slot, pos, c], sem).start()
            pltpu.make_async_copy(all_.at[u, :, 1 - c], to.at[slot, :, 1 - c], sem).start()

    def loaded(slot):
        for i, (all_, to) in enumerate(((g_ref, guv), (d_ref, wdv))):
            pltpu.make_async_copy(all_.at[0], to.at[slot], load_sem.at[slot, i]).wait()

    def gate_half(slot, which, half):
        w = guv[slot, :, :, which, :, pl.ds(512 * half, 512)]
        return w.reshape(width, 512)

    def down_half(slot, half):
        return wdv[slot, pl.ds(2 * half, 2)].reshape(512, width)

    def io(src, dst):
        copy = pltpu.make_async_copy(src, dst, io_sem)
        copy.start()
        copy.wait()

    def tile(m):
        return pl.ds(pl.multiple_of(m * rows, rows), rows)

    def scale_of(h):
        wide = h.astype(F32)
        return wide, lax.rsqrt(jnp.mean(wide * wide, -1, keepdims=True) + 1e-6)

    def put_normed(m, h, plain, turned):
        wide, scale = scale_of(h)
        out = (wide * scale).astype(BF)
        if plain:
            a[tile(m), :] = out
        if turned:
            at[:, tile(m)] = out.T

    def norm_back(m, h):
        wide, scale = scale_of(h)
        by_a = acc[tile(m), :].astype(BF).astype(F32)
        by_scale = jnp.sum(by_a * wide, -1, keepdims=True)
        by_h = by_a * scale - wide * (scale * scale * scale * by_scale * (1.0 / width))
        return (dy[tile(m), :].astype(F32) + by_h.astype(BF).astype(F32)).astype(BF)

    def add(to, term_):
        to[...] = (to[...].astype(F32) + term_[...].astype(F32)).astype(BF)

    H = 384

    def c1(slot):
        return remote(term.at[1 - c], r1.at[slot], s1.at[0, slot], s1.at[1, slot], dev_p)

    def c2(slot):
        return (
            remote(r1.at[slot, 1 - x, :, :, pl.ds(0, H)], r2.at[slot, 0], s2.at[0, slot, 0], s2.at[1, slot, 0], dev_x),
            remote(r1.at[slot, :, 1 - y, :, pl.ds(H, H)], r2.at[slot, 1], s2.at[0, slot, 1], s2.at[1, slot, 1], dev_y),
        )

    def c3(slot):
        return (
            remote(r2.at[slot, 0, 1 - y], r3.at[slot, 0], s3.at[0, slot, 0], s3.at[1, slot, 0], dev_y),
            remote(r2.at[slot, 1, 1 - x], r3.at[slot, 1], s3.at[0, slot, 1], s3.at[1, slot, 1], dev_x),
        )

    def c4(slot):
        return remote(r3.at[slot], r4.at[slot], s4.at[0, slot], s4.at[1, slot], dev_z)

    def written(slot):
        return pltpu.make_async_copy(r4.at[slot], out_ref.at[0], out_sem.at[slot])

    def stage1(t):
        slot = t % 2
        c1(slot).wait()
        for i in range(2):
            for k in range(2):
                add(r1.at[slot, i, k], term.at[c, i, k])
        for copy in c2(slot):
            copy.start()

    def stage2(t):
        slot = t % 2
        for copy in c2(slot):
            copy.wait()
        for k in range(2):
            add(r2.at[slot, 0, k], r1.at[slot, x, k, :, pl.ds(0, H)])
            add(r2.at[slot, 1, k], r1.at[slot, k, y, :, pl.ds(H, H)])
        for copy in c3(slot):
            copy.start()

    def stage3(t):
        slot = t % 2
        for copy in c3(slot):
            copy.wait()
        add(r3.at[slot, 0], r2.at[slot, 0, y])
        add(r3.at[slot, 1], r2.at[slot, 1, x])
        c4(slot).start()

    def stage4(t):
        slot = t % 2
        c4(slot).wait()
        add(r4.at[slot], r3.at[slot])
        u = (t + J) % U
        pltpu.make_async_copy(r4.at[slot], out_ref.at[u], out_sem.at[slot]).start()

    def early(t):
        @pl.when((t >= 3) & (t < U + 3))
        def _():
            written((t - 3) % 2).wait()

        @pl.when((t >= 2) & (t < U + 2))
        def _():
            stage3(t - 2)

        @pl.when((t >= 1) & (t < U + 1))
        def _():
            stage1(t - 1)

    def late(t):
        @pl.when((t >= 2) & (t < U + 2))
        def _():
            stage4(t - 2)

        @pl.when((t >= 1) & (t < U + 1))
        def _():
            stage2(t - 1)

        @pl.when(t < U)
        def _():
            c1(t % 2).start()

    barrier = pltpu.get_barrier_semaphore()
    for dev in (dev_p, dev_x, dev_y, dev_z):
        pl.semaphore_signal(barrier, inc=1, device_id=dev, device_id_type=MESH)
    pl.semaphore_wait(barrier, 4)

    @pl.loop(0, U)
    def _(u):
        hop(u)

    io(x_ref, dy)

    @pl.loop(0, TILES)
    def _(m):
        put_normed(m, dy[tile(m), :], True, False)
        acc[tile(m), :] = jnp.zeros((rows, width), F32)

    forward(0)
    forward(1)
    across(0)
    arrived(0)
    load(0, 0)

    @pl.loop(0, J)
    def _(u):
        slot = u % 2
        loaded(slot)

        def part(half, start, stop):
            @pl.loop(start, stop)
            def _(m):
                gate = nn(a[tile(m), :], gate_half(slot, 0, half))
                up = nn(a[tile(m), :], gate_half(slot, 1, half))
                hidden = (gate * jax.nn.sigmoid(gate) * up).astype(BF)
                acc[tile(m), :] += nn(hidden, down_half(slot, half))

        part(0, 0, TILES)
        forward(u + 2)
        across(u + 1)
        part(1, 0, TILES)
        arrived(u + 1)
        load(u + 1, 1 - slot)

    @pl.loop(0, TILES)
    def _(m):
        h = (dy[tile(m), :].astype(F32) + acc[tile(m), :].astype(BF).astype(F32)).astype(BF)
        dy[tile(m), :] = h
        put_normed(m, h, True, True)
        acc[tile(m), :] = jnp.zeros((rows, width), F32)

    io(dy, h_ref)
    io(dy_ref, dy)

    @pl.loop(0, TILES)
    def _(m):
        dyt[:, tile(m)] = dy[tile(m), :].T

    @pl.loop(0, U)
    def _(t):
        slot = t % 2

        @pl.when(t == J)
        def _():
            io(h_ref, a)

            @pl.loop(0, TILES)
            def _(m):
                out = norm_back(m, a[tile(m), :])
                dy[tile(m), :] = out
                dyt[:, tile(m)] = out.T
                acc[tile(m), :] = jnp.zeros((rows, width), F32)

            io(x_ref, a)

            @pl.loop(0, TILES)
            def _(m):
                put_normed(m, a[tile(m), :], True, True)

        loaded(slot)

        def hidden(half):
            @pl.loop(0, TILES)
            def _(m):
                gate = nn(a[tile(m), :], gate_half(slot, 0, half))
                up = nn(a[tile(m), :], gate_half(slot, 1, half))
                by_mid = nt(dy[tile(m), :], down_half(slot, half)).astype(BF).astype(F32)
                sig = jax.nn.sigmoid(gate)
                silu = gate * sig
                mid[tile(m), :] = (silu * up).astype(BF)
                du[tile(m), :] = (by_mid * silu).astype(BF)
                dg[tile(m), :] = (by_mid * up * (sig + silu * (1.0 - sig))).astype(BF)

        def weights(half):
            @pl.loop(0, 2)
            def _(n):
                cols = pl.ds(pl.multiple_of(n * 256, 256), 256)
                for which, of in enumerate((dg, du)):
                    out = nn(at[...], of[:, cols]).astype(BF)
                    for k in range(2):
                        place = pl.ds(pl.multiple_of(96 * (4 * half + k) + 192 * n, 32), 96)
                        for to in range(8):
                            term[to % 2, to // 4, (to // 2) % 2, which, place, :] = out[96 * to : 96 * to + 96, 128 * k : 128 * k + 128]
                out = nn(dyt[...], mid[:, cols]).astype(BF)
                for k in range(2):
                    term[k, half, n, 2] = out[:, 128 * k : 128 * k + 128]

        def states(half):
            @pl.loop(0, TILES)
            def _(m):
                acc[tile(m), :] += nt(dg[tile(m), :], gate_half(slot, 0, half)) + nt(du[tile(m), :], gate_half(slot, 1, half))

        hidden(0)
        early(t)

        @pl.when(t < 2)
        def _():
            forward(J + 2 + 2 * t)

        @pl.when(t < 3)
        def _():
            across(J + 1 + 2 * t)

        weights(0)
        states(0)

        @pl.when(t < J - 1)
        def _():
            arrived(J + 1 + t)

        @pl.when(t < U - 1)
        def _():
            load((J + 1 + t) % U, 1 - slot)

        @pl.when(t < 2)
        def _():
            forward(J + 3 + 2 * t)
            across(J + 2 + 2 * t)

        hidden(1)
        weights(1)
        late(t)
        states(1)

    early(U)
    io(x_ref, a)

    @pl.loop(0, TILES)
    def _(m):
        dy[tile(m), :] = norm_back(m, a[tile(m), :])

    io(dy, dx_ref)
    late(U)
    early(U + 1)
    late(U + 1)
    early(U + 2)
    for u in range(U):
        sent(u)


def solution(mesh):
    def step(x, dy, w_gate, w_up, w_down):
        tokens, width = x.shape[1:]
        layers, own, ff = w_gate.shape
        U = layers * J

        def chunked(w):
            return w.reshape(layers, own, 8, J, 128).transpose(0, 3, 1, 2, 4).reshape(U, own, 1024)

        gu = jnp.stack([chunked(w_gate), chunked(w_up)], 1)
        wd = w_down.reshape(U, 128, width)
        hbm = pl.BlockSpec(memory_space=pl.ANY)
        vmem, dma = pltpu.VMEM, pltpu.SemaphoreType.DMA
        dx, out, *_ = pl.pallas_call(
            kernel,
            in_specs=[hbm] * 4,
            out_specs=[hbm] * 5,
            out_shape=[
                jax.ShapeDtypeStruct((tokens, width), BF),
                jax.ShapeDtypeStruct((U, 2, 3, 384, 128), BF),
                jax.ShapeDtypeStruct((U, 4, 2, 2, own, 1024), BF),
                jax.ShapeDtypeStruct((U, 4, 2, 128, width), BF),
                jax.ShapeDtypeStruct((tokens, width), BF),
            ],
            scratch_shapes=[
                vmem((tokens, width), BF),
                vmem((width, tokens), BF),
                vmem((tokens, width), BF),
                vmem((width, tokens), BF),
                vmem((tokens, width), F32),
                vmem((2, 4, 2, 2, own, 1024), BF),
                vmem((2, 4, 2, 128, width), BF),
                vmem((tokens, 512), BF),
                vmem((tokens, 512), BF),
                vmem((tokens, 512), BF),
                vmem((2, 2, 2, 3, 768, 128), BF),
                vmem((2, 2, 2, 3, 768, 128), BF),
                vmem((2, 2, 2, 3, 384, 128), BF),
                vmem((2, 2, 3, 384, 128), BF),
                vmem((2, 2, 3, 384, 128), BF),
                dma((U, 4, 2)),
                dma((U, 2, 2)),
                dma((2, 2)),
                dma((2, 2)),
                dma((2, 2, 2)),
                dma((2, 2, 2)),
                dma((2, 2)),
                dma((2,)),
                dma,
            ],
            compiler_params=pltpu.CompilerParams(collective_id=0, has_side_effects=True, vmem_limit_bytes=67043328),
            name="stack",
        )(x[0], dy[0], gu, wd)
        out = out.reshape(layers, J, 2, 3, 4, own, 128)

        def rows_of(which):
            return out[:, :, :, which].transpose(0, 4, 2, 3, 1, 5).reshape(layers, own, ff)

        down = out[:, :, :, 2].reshape(layers, J, width, 128).transpose(0, 1, 3, 2).reshape(layers, J * 128, width)
        return dx[None], rows_of(0), rows_of(1), down

    states, cut = P(("rep", "r", "s"), None, None), P(None, "s", None)
    return jax.shard_map(
        step,
        mesh=mesh,
        in_specs=(states, states) + (cut,) * 3,
        out_specs=(states,) + (P("rep", "s", None),) * 3,
        check_vma=False,
    )
```

```python
import functools

import jax
import jax.numpy as jnp
from jax import lax
from jax.experimental import pallas as pl
from jax.experimental.pallas import tpu as pltpu
from jax.sharding import PartitionSpec as P

MESH = pl.DeviceIdType.MESH
BF, F32 = jnp.bfloat16, jnp.float32
J = 6
TILES = 4


def nn(a, b):
    return lax.dot_general(a, b, (((1,), (0,)), ((), ())), preferred_element_type=F32)


def nt(a, b):
    return lax.dot_general(a, b, (((1,), (1,)), ((), ())), preferred_element_type=F32)


def kernel(
    x_ref, dy_ref, wg_ref, wu_ref, wd_ref,
    dx_ref, dwg_ref, dwu_ref, dwd_ref, g_ref, d_ref, h_ref, save_ref, mid_ref,
    a, at, dy, dyt, acc, guv, wdv, mid, dgu, term, r1, r2, r3, r4, shard, turned, pair,
    ag_recv, ag_send, load_sem, s1, s2, s3, s4, out_sem, io_sem, shard_sem, save_sem, mid_sem,
):
    tokens, width = a.shape
    rows = tokens // TILES
    U = 2 * J
    r, s = lax.axis_index("r"), lax.axis_index("s")
    c, y, x = s % 2, (s // 2) % 2, s // 4
    xy = s // 2
    partner, xn, yn = s + 1 - 2 * c, s + 4 - 8 * x, s + 2 - 4 * y
    dev_p, dev_x, dev_y, dev_z = {"s": partner}, {"s": xn}, {"s": yn}, {"r": 1 - r}
    dev_1 = {"s": xn * (1 - r) + yn * r}
    dev_2 = {"s": xn * r + yn * (1 - r)}
    pos1 = xy + (1 - r) * (2 - 4 * x) + r * (1 - 2 * y)
    pos2 = xy + r * (2 - 4 * x) + (1 - r) * (1 - 2 * y)
    pos3 = 3 - xy

    def remote(src, dst, send, recv, dev):
        return pltpu.make_async_remote_copy(src_ref=src, dst_ref=dst, send_sem=send, recv_sem=recv, device_id=dev, device_id_type=MESH)

    def down_own(u):
        return wd_ref.at[u // J, pl.ds(pl.multiple_of(128 * (u % J), 128), 128)]

    def pieces(u, pos, own):
        return (g_ref.at[u, pos, c], down_own(u) if own else d_ref.at[u, pos, c])

    def send_block(u, pos, own, kind, dev):
        for i, (src, dst) in enumerate(zip(pieces(u, pos, own), (g_ref.at[u, pos, c], d_ref.at[u, pos, c]))):
            remote(src, dst, ag_send.at[u, 1 if kind == 3 else 0, i], ag_recv.at[u, kind, i], dev).start()

    def wait_block(u, pos, kind):
        for i, ref in enumerate((g_ref.at[u, pos, c], d_ref.at[u, pos, c])):
            remote(ref, ref, ag_send.at[u, 0, i], ag_recv.at[u, kind, i], dev_1).wait_recv()

    def hop(u):
        send_block(u, xy, True, 0, dev_1)

    def forward(u):
        send_block(u, xy, True, 3, dev_p)
        wait_block(u, pos1, 0)
        send_block(u, pos1, False, 1, dev_2)
        send_block(u, pos1, False, 2, dev_z)
        send_block(u, pos1, False, 3, dev_p)

    def across(u):
        wait_block(u, pos2, 2)
        send_block(u, pos2, False, 3, dev_p)
        wait_block(u, pos3, 1)
        send_block(u, pos3, False, 3, dev_p)

    def arrived(u):
        for i, ref in enumerate((g_ref.at[u, :, 1 - c], d_ref.at[u, :, 1 - c])):
            remote(ref, ref, ag_send.at[u, 1, i], ag_recv.at[u, 3, i], dev_p).wait_recv()

    def sent(u):
        for i, ref in enumerate((g_ref, d_ref)):
            three, four = ref.at[u, pl.ds(0, 3), 0], ref.at[u, :, 0]
            remote(three, three, ag_send.at[u, 0, i], ag_recv.at[u, 0, i], dev_1).wait_send()
            remote(four, four, ag_send.at[u, 1, i], ag_recv.at[u, 3, i], dev_p).wait_send()

    def load(u, slot):
        pltpu.make_async_copy(g_ref.at[u], guv.at[slot], load_sem.at[slot, 0]).start()
        sem = load_sem.at[slot, 1]
        pltpu.make_async_copy(down_own(u), wdv.at[slot, xy, c], sem).start()
        for pos in (pos1, pos2, pos3):
            pltpu.make_async_copy(d_ref.at[u, pos, c], wdv.at[slot, pos, c], sem).start()
        pltpu.make_async_copy(d_ref.at[u, :, 1 - c], wdv.at[slot, :, 1 - c], sem).start()

    def loaded(slot):
        for i, (all_, to) in enumerate(((g_ref, guv), (d_ref, wdv))):
            pltpu.make_async_copy(all_.at[0], to.at[slot], load_sem.at[slot, i]).wait()

    def gate_half(slot, which, half):
        w = guv[slot, :, :, which, :, pl.ds(512 * half, 512)]
        return w.reshape(width, 512)

    def down_half(slot, half):
        return wdv[slot, pl.ds(2 * half, 2)].reshape(512, width)

    def io(src, dst):
        copy = pltpu.make_async_copy(src, dst, io_sem)
        copy.start()
        copy.wait()

    def tile(m):
        return pl.ds(pl.multiple_of(m * rows, rows), rows)

    def scale_of(h):
        wide = h.astype(F32)
        return wide, lax.rsqrt(jnp.mean(wide * wide, -1, keepdims=True) + 1e-6)

    def put_normed(m, h, plain, turned):
        wide, scale = scale_of(h)
        out = (wide * scale).astype(BF)
        if plain:
            a[tile(m), :] = out
        if turned:
            at[:, tile(m)] = out.T

    def norm_back(m, h):
        wide, scale = scale_of(h)
        by_a = acc[tile(m), :].astype(BF).astype(F32)
        by_scale = jnp.sum(by_a * wide, -1, keepdims=True)
        by_h = by_a * scale - wide * (scale * scale * scale * by_scale * (1.0 / width))
        return (dy[tile(m), :].astype(F32) + by_h.astype(BF).astype(F32)).astype(BF)

    def add(to, term_):
        to[...] = (to[...].astype(F32) + term_[...].astype(F32)).astype(BF)

    H = 384

    def c1(slot):
        return remote(term.at[1 - c], r1.at[slot], s1.at[0, slot], s1.at[1, slot], dev_p)

    def c2(slot):
        return (
            remote(r1.at[slot, 1 - x, :, :, pl.ds(0, H)], r2.at[slot, 0], s2.at[0, slot, 0], s2.at[1, slot, 0], dev_x),
            remote(r1.at[slot, :, 1 - y, :, pl.ds(H, H)], r2.at[slot, 1], s2.at[0, slot, 1], s2.at[1, slot, 1], dev_y),
        )

    def c3(slot):
        return (
            remote(r2.at[slot, 0, 1 - y], r3.at[slot, 0], s3.at[0, slot, 0], s3.at[1, slot, 0], dev_y),
            remote(r2.at[slot, 1, 1 - x], r3.at[slot, 1], s3.at[0, slot, 1], s3.at[1, slot, 1], dev_x),
        )

    def c4(slot):
        return remote(r3.at[slot], r4.at[slot], s4.at[0, slot], s4.at[1, slot], dev_z)

    def written(slot, u=0):
        return pltpu.make_async_copy(turned.at[slot], down_grad(u), out_sem.at[slot])

    def down_grad(u):
        return dwd_ref.at[u // J, pl.ds(pl.multiple_of(128 * (u % J), 128), 128)]

    def layer_written(layer):
        return [pltpu.make_async_copy(shard.at[layer, i], to.at[layer], shard_sem.at[layer, i]) for i, to in enumerate((dwg_ref, dwu_ref))]

    def stage1(t):
        slot = t % 2
        c1(slot).wait()
        for i in range(2):
            for k in range(2):
                add(r1.at[slot, i, k], term.at[c, i, k])
        for copy in c2(slot):
            copy.start()

    def stage2(t):
        slot = t % 2
        for copy in c2(slot):
            copy.wait()
        for k in range(2):
            add(r2.at[slot, 0, k], r1.at[slot, x, k, :, pl.ds(0, H)])
            add(r2.at[slot, 1, k], r1.at[slot, k, y, :, pl.ds(H, H)])
        for copy in c3(slot):
            copy.start()

    def stage3(t):
        slot = t % 2
        for copy in c3(slot):
            copy.wait()
        add(r3.at[slot, 0], r2.at[slot, 0, y])
        add(r3.at[slot, 1], r2.at[slot, 1, x])
        c4(slot).start()

    def stage4(t):
        slot = t % 2
        c4(slot).wait()
        u = (t + J) % U
        for half in range(2):
            for i in range(2):
                for k in range(4):
                    own = pl.ds(96 * k, 96)
                    total = r4[slot, half, i, own].astype(F32) + r3[slot, half, i, own].astype(F32)
                    lanes = pl.ds(pl.multiple_of(768 * (4 * half + k) + 128 * (u % J), 128), 128)
                    shard[u // J, i, :, lanes] = total.astype(BF)
            total = r4[slot, half, 2].astype(F32) + r3[slot, half, 2].astype(F32)
            turned[slot, :, H * half : H * half + H] = total.astype(BF).T
        written(slot, u).start()

        @pl.when(u % J == J - 1)
        def _():
            for copy in layer_written(u // J):
                copy.start()

    def early(t):
        @pl.when((t >= 3) & (t < U + 3))
        def _():
            written((t - 3) % 2).wait()

        @pl.when((t >= 2) & (t < U + 2))
        def _():
            stage3(t - 2)

        @pl.when((t >= 1) & (t < U + 1))
        def _():
            stage1(t - 1)

    def late(t):
        @pl.when((t >= 2) & (t < U + 2))
        def _():
            stage4(t - 2)

        @pl.when((t >= 1) & (t < U + 1))
        def _():
            stage2(t - 1)

        @pl.when(t < U)
        def _():
            c1(t % 2).start()

    barrier = pltpu.get_barrier_semaphore()
    for dev in (dev_p, dev_x, dev_y, dev_z):
        pl.semaphore_signal(barrier, inc=1, device_id=dev, device_id_type=MESH)
    pl.semaphore_wait(barrier, 4)

    def fetched(layer):
        return [pltpu.make_async_copy(ref.at[layer], shard.at[layer, i], shard_sem.at[layer, i]) for i, ref in enumerate((wg_ref, wu_ref))]

    fetching = [copy for layer in range(2) for copy in fetched(layer)]
    for copy in fetching:
        copy.start()
    getting = pltpu.make_async_copy(x_ref, dy, io_sem)
    getting.start()

    for layer in range(2):
        for i in range(2):
            fetching[2 * layer + i].wait()

        @pl.loop(0, J)
        def _(j):
            u = J * layer + j
            block = guv.at[u // 8, (u // 2) % 4, u % 2]
            for i in range(2):
                for k in range(8):
                    lanes = pl.ds(pl.multiple_of(768 * k + 128 * j, 128), 128)
                    block[i, :, 128 * k : 128 * k + 128] = shard[layer, i, :, lanes]

        puts = []
        for u in range(J * layer, J * layer + J):
            puts.append(pltpu.make_async_copy(guv.at[u // 8, (u // 2) % 4, u % 2], g_ref.at[u, xy, c], save_sem.at[u]))
            puts[-1].start()
        for u in range(J * layer, J * layer + J):
            puts[u - J * layer].wait()
            hop(u)

    getting.wait()

    @pl.loop(0, TILES)
    def _(m):
        put_normed(m, dy[tile(m), :], True, False)
        acc[tile(m), :] = jnp.zeros((rows, width), F32)

    forward(0)
    forward(1)
    across(0)
    arrived(0)
    load(0, 0)

    def saved(u, half, m):
        return (
            pltpu.make_async_copy(pair.at[m % 2], save_ref.at[u, half, m], save_sem.at[m % 2]),
            pltpu.make_async_copy(mid.at[tile(m)], mid_ref.at[u, half, tile(m)], mid_sem.at[m % 2]),
        )

    def restored(u, half, m):
        return pltpu.make_async_copy(save_ref.at[u, half, m], pair.at[m % 2], save_sem.at[m % 2])

    @pl.loop(0, J)
    def _(u):
        slot = u % 2
        loaded(slot)

        def part(half, start, stop):
            @pl.loop(start, stop)
            def _(m):
                gate = nn(a[tile(m), :], gate_half(slot, 0, half))
                up = nn(a[tile(m), :], gate_half(slot, 1, half))

                @pl.when((u > 0) | (m >= 2) | (half > 0))
                def _():
                    for copy in saved(u, half, m):
                        copy.wait()

                sig = jax.nn.sigmoid(gate)
                silu = gate * sig
                hidden = (silu * up).astype(BF)
                mid[tile(m), :] = hidden
                pair[m % 2, 0] = silu
                pair[m % 2, 1] = up * (sig + silu * (1.0 - sig))
                acc[tile(m), :] += nn(hidden, down_half(slot, half))
                for copy in saved(u, half, m):
                    copy.start()

        part(0, 0, TILES)
        forward(u + 2)
        across(u + 1)
        part(1, 0, TILES)
        arrived(u + 1)
        load(u + 1, 1 - slot)

    for m in range(2):
        for copy in saved(0, 0, m):
            copy.wait()

    @pl.loop(0, TILES)
    def _(m):
        h = (dy[tile(m), :].astype(F32) + acc[tile(m), :].astype(BF).astype(F32)).astype(BF)
        dy[tile(m), :] = h
        put_normed(m, h, True, True)
        acc[tile(m), :] = jnp.zeros((rows, width), F32)

    io(dy, h_ref)
    io(dy_ref, dy)

    @pl.loop(0, TILES)
    def _(m):
        dyt[:, tile(m)] = dy[tile(m), :].T

    @pl.loop(0, U)
    def _(t):
        slot = t % 2

        @pl.when(t == J)
        def _():
            io(h_ref, a)

            @pl.loop(0, TILES)
            def _(m):
                out = norm_back(m, a[tile(m), :])
                dy[tile(m), :] = out
                dyt[:, tile(m)] = out.T
                acc[tile(m), :] = jnp.zeros((rows, width), F32)

            io(x_ref, a)

            @pl.loop(0, TILES)
            def _(m):
                put_normed(m, a[tile(m), :], False, True)

            for m in range(2):
                restored(0, 0, m).start()

        loaded(slot)

        def hidden(half):
            @pl.loop(0, TILES)
            def _(m):
                gate = nn(a[tile(m), :], gate_half(slot, 0, half))
                up = nn(a[tile(m), :], gate_half(slot, 1, half))
                by_mid = nt(dy[tile(m), :], down_half(slot, half)).astype(BF).astype(F32)
                sig = jax.nn.sigmoid(gate)
                silu = gate * sig
                mid[tile(m), :] = (silu * up).astype(BF)
                dgu[tile(m), 0:512] = (by_mid * (up * (sig + silu * (1.0 - sig)))).astype(BF)
                dgu[tile(m), 512:1024] = (by_mid * silu).astype(BF)

        def restore(half):
            u = t - J
            getting = pltpu.make_async_copy(mid_ref.at[u, half], mid, mid_sem.at[0])
            getting.start()

            @pl.loop(0, TILES)
            def _(m):
                by_mid = nt(dy[tile(m), :], down_half(slot, half)).astype(BF).astype(F32)
                restored(u, half, m).wait()
                dgu[tile(m), 0:512] = (by_mid * pair[m % 2, 1]).astype(BF)
                dgu[tile(m), 512:1024] = (by_mid * pair[m % 2, 0]).astype(BF)

                @pl.when(m < 2)
                def _():
                    restored(u, half, m + 2).start()

                @pl.when((m >= 2) & ((u < J - 1) | (half == 0)))
                def _():
                    restored(u + half, 1 - half, m - 2).start()

            getting.wait()

        def products(half):
            @pl.when(t < J)
            def _():
                hidden(half)

            @pl.when(t >= J)
            def _():
                restore(half)

        def weights(half):
            @pl.loop(0, 2)
            def _(n):
                cols = pl.ds(pl.multiple_of(n * 256, 256), 256)
                for which in range(2):
                    out = nn(at[...], dgu[:, pl.ds(pl.multiple_of(512 * which + n * 256, 256), 256)]).astype(BF)
                    for k in range(2):
                        place = pl.ds(pl.multiple_of(96 * (4 * half + k) + 192 * n, 32), 96)
                        for to in range(8):
                            term[to % 2, to // 4, (to // 2) % 2, which, place, :] = out[96 * to : 96 * to + 96, 128 * k : 128 * k + 128]
                out = nn(dyt[...], mid[:, cols]).astype(BF)
                for k in range(2):
                    term[k, half, n, 2] = out[:, 128 * k : 128 * k + 128]

        def states(half):
            @pl.loop(0, TILES)
            def _(m):
                both = jnp.concatenate([gate_half(slot, 0, half), gate_half(slot, 1, half)], 1)
                acc[tile(m), :] += nt(dgu[tile(m), :], both)

        products(0)
        early(t)

        @pl.when(t < 2)
        def _():
            forward(J + 2 + 2 * t)

        @pl.when(t < 3)
        def _():
            across(J + 1 + 2 * t)

        weights(0)
        states(0)

        @pl.when(t < J - 1)
        def _():
            arrived(J + 1 + t)

        @pl.when(t < U - 1)
        def _():
            load((J + 1 + t) % U, 1 - slot)

        @pl.when(t < 2)
        def _():
            forward(J + 3 + 2 * t)
            across(J + 2 + 2 * t)

        products(1)
        weights(1)
        late(t)
        states(1)

    early(U)

    @pl.loop(0, TILES)
    def _(m):
        dy[tile(m), :] = norm_back(m, a[tile(m), :])

    io(dy, dx_ref)
    late(U)
    early(U + 1)
    late(U + 1)
    early(U + 2)
    for layer in range(2):
        for copy in layer_written(layer):
            copy.wait()

    @pl.loop(0, U)
    def _(u):
        sent(u)


def solution(mesh):
    def step(x, dy, w_gate, w_up, w_down):
        tokens, width = x.shape[1:]
        layers, own, ff = w_gate.shape
        U = layers * J

        hbm = pl.BlockSpec(memory_space=pl.ANY)
        vmem, dma = pltpu.VMEM, pltpu.SemaphoreType.DMA
        dx, by_gate, by_up, by_down, *_ = pl.pallas_call(
            kernel,
            in_specs=[hbm] * 5,
            out_specs=[hbm] * 9,
            out_shape=[
                jax.ShapeDtypeStruct((tokens, width), BF),
                *(jax.ShapeDtypeStruct(w.shape, BF) for w in (w_gate, w_up, w_down)),
                jax.ShapeDtypeStruct((U, 4, 2, 2, own, 1024), BF),
                jax.ShapeDtypeStruct((U, 4, 2, 128, width), BF),
                jax.ShapeDtypeStruct((tokens, width), BF),
                jax.ShapeDtypeStruct((J, 2, TILES, 2, tokens // TILES, 512), F32),
                jax.ShapeDtypeStruct((J, 2, tokens, 512), BF),
            ],
            scratch_shapes=[
                vmem((tokens, width), BF),
                vmem((width, tokens), BF),
                vmem((tokens, width), BF),
                vmem((width, tokens), BF),
                vmem((tokens, width), F32),
                vmem((2, 4, 2, 2, own, 1024), BF),
                vmem((2, 4, 2, 128, width), BF),
                vmem((tokens, 512), BF),
                vmem((tokens, 1024), BF),
                vmem((2, 2, 2, 3, 768, 128), BF),
                vmem((2, 2, 2, 3, 768, 128), BF),
                vmem((2, 2, 2, 3, 384, 128), BF),
                vmem((2, 2, 3, 384, 128), BF),
                vmem((2, 2, 3, 384, 128), BF),
                vmem((layers, 2, own, ff), BF),
                vmem((2, 128, width), BF),
                vmem((2, 2, tokens // TILES, 512), F32),
                dma((U, 4, 2)),
                dma((U, 2, 2)),
                dma((2, 2)),
                dma((2, 2)),
                dma((2, 2, 2)),
                dma((2, 2, 2)),
                dma((2, 2)),
                dma((2,)),
                dma,
                dma((2, 2)),
                dma((U,)),
                dma((2,)),
            ],
            compiler_params=pltpu.CompilerParams(collective_id=0, has_side_effects=True, vmem_limit_bytes=67043328),
            name="stack",
        )(x[0], dy[0], w_gate, w_up, w_down)
        return dx[None], by_gate, by_up, by_down

    states, cut = P(("rep", "r", "s"), None, None), P(None, "s", None)
    return jax.shard_map(
        step,
        mesh=mesh,
        in_specs=(states, states) + (cut,) * 3,
        out_specs=(states,) + (P("rep", "s", None),) * 3,
        check_vma=False,
    )
```
